32 devices in a mesh: rep: 4 (over x, core), shard: 8 (over z, y).
Axes of the slice: x: 2, y: 2, z: 4, core: 2. Of those that a mesh axis runs over, the one named last changes fastest.
Arguments:
- images: bfloat16 [32, 256, 1152], P(('rep', 'shard')), may hold values from -6 to 6
- cotangent: bfloat16 [32, 256, 1152], P(('rep', 'shard')), may hold values from -6 to 6
- w_qkv: bfloat16 [1152, 3456], P('shard'), may hold values from -2 to 2
- w_out: bfloat16 [1152, 1152], P('shard'), may hold values from -0.75 to 0.75
- w_up: bfloat16 [1152, 4304], P('shard'), may hold values from -0.1875 to 0.1875
- w_down: bfloat16 [1152, 4304], P('shard'), may hold values from -0.125 to 0.125
- vectors: bfloat16 [1152, 8], P('shard'), may hold values from -3 to 3, as said below
- up_bias: bfloat16 [4304], replicated, may hold values from -3 to 3
Outputs:
- outputs: bfloat16 [32, 256, 1152], P(('rep', 'shard'))
- input_grad: bfloat16 [32, 256, 1152], P(('rep', 'shard'))
- qkv_grad: float32 [1152, 3456], P('shard')
- out_grad: float32 [1152, 1152], P('shard')
- up_grad: float32 [1152, 4304], P('shard')
- down_grad: float32 [1152, 4304], P('shard')
- vectors_grad: float32 [1152, 8], P('shard')
- up_bias_grad: float32 [4304], replicated
The draws below stay inside these ranges and needn't reach their ends.
Inputs may be any that keep to these rules, and one draw needn't show every extreme that they name: `vectors`: columns 0 and 5 (the norms' gains) are positive; the other columns have either sign.
All inputs are finite; a program needn't handle non-finite values.
Results may differ from the reference program's by a relative error of at most 0.014.
Values may be sent and summed in bfloat16 or wider, within the bound.
A program may use at most 256 MiB of HBM per device.

```python
import math
import jax
import jax.numpy as jnp
from jax import lax

D = 1152
HEAD_DIM = 72
FF = 4304
SEQ = 256
IMAGES = 32


def draw_vectors(key, part):
    key_shift = jax.random.fold_in(key, 11)
    key_gain = jax.random.fold_in(key, 12)
    shifts = jnp.clip(0.5 * jax.random.normal(key_shift, (D, 8), jnp.float32), -3.0, 3.0)
    upper = jnp.full((8,), math.log(2.0), jnp.float32)
    lower = jnp.full((8,), math.log(0.5), jnp.float32)
    fraction = jax.random.uniform(key_gain, (D, 8), jnp.float32)
    gains = jnp.exp(lower + (upper - lower) * fraction)
    column = jnp.arange(8)
    is_gain = (column == 0) | (column == 5)
    return jnp.where(is_gain[None, :], gains, shifts).astype(jnp.bfloat16)


def draw_w_qkv(key, part):
    key_entries = jax.random.fold_in(key, 21)
    entries = jnp.clip(jax.random.normal(key_entries, (D, 3 * D), jnp.float32), -4.0, 4.0) / math.sqrt(D)
    return entries.astype(jnp.bfloat16)


def level_of(key, shape, cuts, smallest, largest):
    def one(position, blocks):
        steps = jax.random.uniform(jax.random.fold_in(jax.random.fold_in(key, 6), position), (blocks,), jnp.float32, smallest / len(cuts), largest / len(cuts))
        return jnp.repeat(jnp.exp(steps), shape[position] // blocks).reshape((-1,) + (1,) * (len(shape) - position - 1))

    level = one(*cuts[0])
    for cut in cuts[1:]:
        level = level * one(*cut)
    return level


def centred(own_key, dims, spread, bound, shards=(), kind=jnp.bfloat16):
    array = spread * jax.random.normal(own_key, dims, jnp.float32)
    if shards:
        array = array * level_of(own_key, dims, shards, -0.22, 0.18)
    return jnp.clip(array, -bound, bound).astype(kind)


def setup_inputs(seed: int = 0) -> dict:
    seeds = jax.random.split(jax.random.key(seed), 9)
    images = centred(seeds[0], (IMAGES, SEQ, D), 1.0, 6.0, ((0, 32),))
    cotangent = centred(seeds[1], (IMAGES, SEQ, D), 1.0, 6.0, ((0, 32),))
    w_qkv = draw_w_qkv(jax.random.fold_in(seeds[8], 71), 0)
    w_out = centred(seeds[3], (D, D), (D // 16) ** -0.5, 0.75, ((0, 8),))
    w_up = centred(seeds[4], (D, FF), D ** -0.5, 0.1875, ((0, 8),))
    w_down = centred(seeds[5], (D, FF), (FF // 2) ** -0.5, 0.125, ((0, 8),))
    vectors = draw_vectors(jax.random.fold_in(seeds[8], 71), 0)
    up_bias = centred(seeds[7], (FF,), 0.5, 3.0)
    return dict(images=images, cotangent=cotangent, w_qkv=w_qkv, w_out=w_out, w_up=w_up, w_down=w_down, vectors=vectors, up_bias=up_bias)


EPSILON = 1e-06
GELU_COEF = 0.044715
ROOT_TWO_PI = math.sqrt(2.0 / math.pi)

def batched(pattern, left_op, right_op):
    return jnp.einsum(pattern, left_op.astype(jnp.float32), right_op.astype(jnp.float32))

def contract_rows(left_op, right_op):
    return lax.dot_general(left_op, right_op, (((0,), (0,)), ((), ())), preferred_element_type=jnp.float32)

def contract_cols(left_op, right_op):
    return lax.dot_general(left_op, right_op, (((1,), (1,)), ((), ())), preferred_element_type=jnp.float32)

def norm_rows(hidden):
    row_mean = lax.optimization_barrier(jnp.mean(hidden, axis=-1, keepdims=True))
    centered = hidden - row_mean
    variance = lax.optimization_barrier(jnp.mean(centered * centered, axis=-1, keepdims=True))
    inv_std = lax.rsqrt(variance + EPSILON)
    return (centered * inv_std, inv_std)

def norm_back(grad_normed, normed, inv_std):
    mean_grad = lax.optimization_barrier(jnp.mean(grad_normed, axis=-1, keepdims=True))
    mean_proj = lax.optimization_barrier(jnp.mean(grad_normed * normed, axis=-1, keepdims=True))
    return inv_std * (grad_normed - mean_grad - normed * mean_proj)

def gelu_parts(pre_act):
    tanh_term = jnp.tanh(ROOT_TWO_PI * (pre_act + GELU_COEF * pre_act * pre_act * pre_act))
    activated = 0.5 * pre_act * (1.0 + tanh_term)
    derivative = 0.5 * (1.0 + tanh_term) + 0.5 * pre_act * (1.0 - tanh_term * tanh_term) * ROOT_TWO_PI * (1.0 + 3.0 * GELU_COEF * pre_act * pre_act)
    return (activated, derivative)

def split_heads(tensor, batch_count, seq_len, head_size):
    return tensor.reshape(batch_count, seq_len, tensor.shape[-1] // head_size, head_size)

def forward_pass(images, w_qkv, w_out, w_up, w_down, vectors, up_bias):
    params = vectors.astype(jnp.float32)
    batch_count, seq_len, model_width = images.shape
    flat_rows = images.reshape(batch_count * seq_len, model_width).astype(jnp.float32)
    normed_one, inv_one = norm_rows(flat_rows)
    input_one = (normed_one * params[:, 0] + params[:, 1]).astype(jnp.bfloat16)
    projected = jnp.dot(input_one, w_qkv, preferred_element_type=jnp.float32)
    query = (projected[:, :model_width] + params[:, 2]).astype(jnp.bfloat16)
    keys_all = projected[:, model_width:2 * model_width].astype(jnp.bfloat16)
    values_all = (projected[:, 2 * model_width:] + params[:, 3]).astype(jnp.bfloat16)
    score_scale = 1.0 / math.sqrt(HEAD_DIM)
    query_heads = split_heads(query, batch_count, seq_len, HEAD_DIM)
    key_heads = split_heads(keys_all, batch_count, seq_len, HEAD_DIM)
    value_heads = split_heads(values_all, batch_count, seq_len, HEAD_DIM)
    scores = batched('bqhd,bkhd->bhqk', query_heads, key_heads) * score_scale
    row_max = lax.optimization_barrier(jnp.max(scores, axis=-1, keepdims=True))
    exponent = jnp.exp(scores - row_max)
    row_total = lax.optimization_barrier(jnp.sum(exponent, axis=-1, keepdims=True))
    weights = (exponent / row_total).astype(jnp.bfloat16)
    logsum = row_max + jnp.log(row_total)
    attended = batched('bhqk,bkhd->bqhd', weights, value_heads).reshape(batch_count * seq_len, model_width).astype(jnp.bfloat16)
    middle = flat_rows + jnp.dot(attended, w_out, preferred_element_type=jnp.float32) + params[:, 4]
    normed_two, inv_two = norm_rows(middle)
    input_two = (normed_two * params[:, 5] + params[:, 6]).astype(jnp.bfloat16)
    pre_act = jnp.dot(input_two, w_up, preferred_element_type=jnp.float32) + up_bias.astype(jnp.float32)
    activated, derivative = gelu_parts(pre_act)
    act_bf = activated.astype(jnp.bfloat16)
    final = middle + contract_cols(act_bf, w_down) + params[:, 7]
    outputs = final.astype(jnp.bfloat16).reshape(batch_count, seq_len, model_width)
    saved = (normed_one, inv_one, input_one, query, keys_all, values_all, logsum, attended, normed_two, inv_two, input_two, derivative, act_bf)
    return (outputs, saved)

def backward_pass(cotangent, saved, w_qkv, w_out, w_up, w_down, vectors):
    normed_one, inv_one, input_one, query, keys_all, values_all, logsum, attended, normed_two, inv_two, input_two, derivative, act_bf = saved
    params = vectors.astype(jnp.float32)
    batch_count, seq_len, model_width = cotangent.shape
    grad_bf = cotangent.reshape(batch_count * seq_len, model_width)
    grad_final = grad_bf.astype(jnp.float32)
    down_term = contract_rows(grad_bf, act_bf)
    grad_act = jnp.dot(grad_bf, w_down, preferred_element_type=jnp.float32)
    grad_pre = grad_act * derivative
    upb_term = lax.optimization_barrier(jnp.sum(grad_pre, axis=0))
    grad_pre_bf = grad_pre.astype(jnp.bfloat16)
    up_term = contract_rows(input_two, grad_pre_bf)
    grad_two = contract_cols(grad_pre_bf, w_up)
    grad_gain_two = lax.optimization_barrier(jnp.sum(grad_two * normed_two, axis=0))
    grad_bias_two = lax.optimization_barrier(jnp.sum(grad_two, axis=0))
    grad_middle = grad_final + norm_back(grad_two * params[:, 5], normed_two, inv_two)
    grad_out_bias = lax.optimization_barrier(jnp.sum(grad_middle, axis=0))
    grad_middle_bf = grad_middle.astype(jnp.bfloat16)
    out_term = contract_rows(attended, grad_middle_bf)
    grad_att = contract_cols(grad_middle_bf, w_out).astype(jnp.bfloat16)
    score_scale = 1.0 / math.sqrt(HEAD_DIM)
    query_heads = split_heads(query, batch_count, seq_len, HEAD_DIM)
    key_heads = split_heads(keys_all, batch_count, seq_len, HEAD_DIM)
    value_heads = split_heads(values_all, batch_count, seq_len, HEAD_DIM)
    grad_heads = split_heads(grad_att, batch_count, seq_len, HEAD_DIM)
    scores = batched('bqhd,bkhd->bhqk', query_heads, key_heads) * score_scale
    probs = jnp.exp(scores - logsum)
    probs_bf = probs.astype(jnp.bfloat16)
    grad_value = batched('bhqk,bqhd->bkhd', probs_bf, grad_heads)
    grad_prob = batched('bqhd,bkhd->bhqk', grad_heads, value_heads)
    delta = lax.optimization_barrier(jnp.sum(probs * grad_prob, axis=-1, keepdims=True))
    grad_score = (probs * (grad_prob - delta) * score_scale).astype(jnp.bfloat16)
    grad_query = batched('bhqk,bkhd->bqhd', grad_score, key_heads)
    grad_key = batched('bhqk,bqhd->bkhd', grad_score, query_heads)
    flat_count = batch_count * seq_len
    grad_query = grad_query.reshape(flat_count, model_width)
    grad_key = grad_key.reshape(flat_count, model_width)
    grad_value = grad_value.reshape(flat_count, model_width)
    grad_qbias = lax.optimization_barrier(jnp.sum(grad_query, axis=0))
    grad_vbias = lax.optimization_barrier(jnp.sum(grad_value, axis=0))
    grad_proj = jnp.concatenate([grad_query, grad_key, grad_value], axis=1).astype(jnp.bfloat16)
    qkv_term = contract_rows(input_one, grad_proj)
    grad_one = contract_cols(grad_proj, w_qkv)
    grad_gain_one = lax.optimization_barrier(jnp.sum(grad_one * normed_one, axis=0))
    grad_bias_one = lax.optimization_barrier(jnp.sum(grad_one, axis=0))
    grad_input = grad_middle + norm_back(grad_one * params[:, 0], normed_one, inv_one)
    grad_down_bias = lax.optimization_barrier(jnp.sum(grad_final, axis=0))
    vector_term = jnp.stack([grad_gain_one, grad_bias_one, grad_qbias, grad_vbias, grad_out_bias, grad_gain_two, grad_bias_two, grad_down_bias], axis=1)
    input_grad = grad_input.astype(jnp.bfloat16).reshape(batch_count, seq_len, model_width)
    return (input_grad, (qkv_term, out_term, up_term, down_term, vector_term), upb_term)

def reference(images, cotangent, w_qkv, w_out, w_up, w_down, vectors, up_bias):
    group = math.gcd(IMAGES, 16)
    image_blocks = images.reshape(IMAGES // group, group, SEQ, D)
    cot_blocks = cotangent.reshape(IMAGES // group, group, SEQ, D)

    def one_block(carry, block_pair):
        image_block, cot_block = block_pair
        outputs, saved = forward_pass(image_block, w_qkv, w_out, w_up, w_down, vectors, up_bias)
        input_grad, terms, upb_term = backward_pass(cot_block, saved, w_qkv, w_out, w_up, w_down, vectors)
        sums, upb_sum = carry
        sums = tuple((total + term for total, term in zip(sums, terms)))
        return ((sums, upb_sum + upb_term), (outputs, input_grad))
    zeros = (jnp.zeros((D, 3 * D), jnp.float32), jnp.zeros((D, D), jnp.float32), jnp.zeros((D, FF), jnp.float32), jnp.zeros((D, FF), jnp.float32), jnp.zeros((D, 8), jnp.float32))
    (sums, upb_sum), (outputs, input_grad) = lax.scan(one_block, (zeros, jnp.zeros((FF,), jnp.float32)), (image_blocks, cot_blocks))
    outputs = outputs.reshape(IMAGES, SEQ, D)
    input_grad = input_grad.reshape(IMAGES, SEQ, D)
    return (outputs, input_grad, sums[0], sums[1], sums[2], sums[3], sums[4], upb_sum)
```

```python
import math

import jax
import jax.numpy as jnp
from jax import lax
from jax.sharding import PartitionSpec as P

HEAD_DIM = 72
EPSILON = 1e-06
GELU_COEF = 0.044715
ROOT_TWO_PI = math.sqrt(2.0 / math.pi)
F32 = jnp.float32
BF16 = jnp.bfloat16


def dot(a, b, ca, cb):
    return lax.dot_general(a, b, (((ca,), (cb,)), ((), ())), preferred_element_type=F32)


def batched(pattern, left_op, right_op):
    return jnp.einsum(pattern, left_op, right_op, preferred_element_type=F32)


def norm_rows(hidden):
    row_mean = jnp.mean(hidden, axis=-1, keepdims=True)
    centered = hidden - row_mean
    variance = jnp.mean(centered * centered, axis=-1, keepdims=True)
    inv_std = lax.rsqrt(variance + EPSILON)
    return (centered * inv_std, inv_std)


def norm_back(grad_normed, normed, inv_std):
    mean_grad = jnp.mean(grad_normed, axis=-1, keepdims=True)
    mean_proj = jnp.mean(grad_normed * normed, axis=-1, keepdims=True)
    return inv_std * (grad_normed - mean_grad - normed * mean_proj)


def gelu_parts(u):
    t = jnp.tanh(ROOT_TWO_PI * (u + GELU_COEF * u * u * u))
    act = 0.5 * u * (1.0 + t)
    der = 0.5 * (1.0 + t) + 0.5 * u * (1.0 - t * t) * ROOT_TWO_PI * (
        1.0 + 3.0 * GELU_COEF * u * u
    )
    return act, der


def gather_rep(a):
    return lax.all_gather(a, "rep", axis=0, tiled=True)


def scatter_rep(a):
    return lax.psum_scatter(a.astype(BF16), "rep", scatter_dimension=0, tiled=True).astype(F32)


def per_device(reps, images, cotangent, w_qkv, w_out, w_up, w_down, vectors, up_bias):
    r = lax.axis_index("rep")
    batch, seq, width = images.shape
    rows = w_qkv.shape[0]
    quarter = width // reps
    ffq = w_up.shape[1] // reps
    heads = quarter // HEAD_DIM

    def take(w, start, size):
        return lax.dynamic_slice_in_dim(w, start, size, 1)

    part = jnp.concatenate(
        [take(w_qkv, t * width + r * quarter, quarter) for t in range(3)], axis=1
    )
    mine_up = take(w_up, r * ffq, ffq)
    mine_down = take(w_down, r * ffq, ffq)
    wq = lax.all_gather(part, "shard", axis=0, tiled=True)
    wo = lax.all_gather(w_out, "shard", axis=0, tiled=True)
    wu = lax.all_gather(mine_up, "shard", axis=0, tiled=True)
    wd = lax.all_gather(mine_down, "shard", axis=0, tiled=True)
    params = lax.all_gather(vectors, "shard", axis=0, tiled=True).astype(F32)
    wo = lax.dynamic_slice_in_dim(wo, r * quarter, quarter, 0)
    bias_up = lax.dynamic_slice_in_dim(up_bias, r * ffq, ffq, 0).astype(F32)

    x = images.reshape(batch * seq, width).astype(F32)
    e = cotangent.reshape(batch * seq, width)
    e_all = gather_rep(e)
    n1, r1 = norm_rows(x)
    a1 = gather_rep((n1 * params[:, 0] + params[:, 1]).astype(BF16))
    proj = dot(a1, wq, 1, 0)
    bq = lax.dynamic_slice_in_dim(params[:, 2], r * quarter, quarter, 0)
    bv = lax.dynamic_slice_in_dim(params[:, 3], r * quarter, quarter, 0)
    group = reps * batch

    def split(t):
        return t.reshape(group, seq, heads, HEAD_DIM)

    q = split((proj[:, :quarter] + bq).astype(BF16))
    k = split(proj[:, quarter : 2 * quarter].astype(BF16))
    v = split((proj[:, 2 * quarter :] + bv).astype(BF16))
    scale = 1.0 / math.sqrt(HEAD_DIM)
    s = batched("bqhd,bkhd->bhqk", q, k) * scale
    top = jnp.max(s, axis=-1, keepdims=True)
    ex = jnp.exp(s - top)
    total = jnp.sum(ex, axis=-1, keepdims=True)
    probs = ex / total
    probs_bf = probs.astype(BF16)
    o = batched("bhqk,bkhd->bqhd", probs_bf, v).reshape(group * seq, quarter).astype(BF16)
    m = x + scatter_rep(dot(o, wo, 1, 0)) + params[:, 4]
    n2, r2 = norm_rows(m)
    a2 = gather_rep((n2 * params[:, 5] + params[:, 6]).astype(BF16))
    act, der = gelu_parts(dot(a2, wu, 1, 0) + bias_up)
    act = act.astype(BF16)
    final = m + scatter_rep(dot(act, wd, 1, 1)) + params[:, 7]
    outputs = final.astype(BF16).reshape(batch, seq, width)

    def reduce_rows(term):
        return lax.psum_scatter(term.astype(BF16), "shard", scatter_dimension=0, tiled=True)

    ef = e.astype(F32)
    g_down = reduce_rows(dot(e_all, act, 0, 0))
    du = dot(e_all, wd, 1, 0) * der
    upb = jnp.sum(du, axis=0)
    dub = du.astype(BF16)
    g_up = reduce_rows(dot(a2, dub, 0, 0))
    da2 = scatter_rep(dot(dub, wu, 1, 1))
    dm = ef + norm_back(da2 * params[:, 5], n2, r2)
    dmb = gather_rep(dm.astype(BF16))
    do = dot(dmb, wo, 1, 1).astype(BF16)
    out_term = dot(o, dmb, 0, 0).astype(BF16)
    out_term = lax.dynamic_update_slice_in_dim(
        jnp.zeros((width, width), BF16), out_term, r * quarter, 0
    )
    g_out = lax.psum_scatter(out_term, "shard", scatter_dimension=0, tiled=True)
    do = split(do)
    dv = batched("bhqk,bqhd->bkhd", probs_bf, do)
    dpr = batched("bqhd,bkhd->bhqk", do, v)
    delta = jnp.sum(probs * dpr, axis=-1, keepdims=True)
    ds = (probs * (dpr - delta) * scale).astype(BF16)
    dq = batched("bhqk,bkhd->bqhd", ds, k)
    dk = batched("bhqk,bqhd->bkhd", ds, q)
    dp = jnp.concatenate([t.reshape(group * seq, quarter) for t in (dq, dk, dv)], axis=1)
    col = jnp.sum(dp, axis=0)
    dp = dp.astype(BF16)
    g_qkv = reduce_rows(dot(a1, dp, 0, 0))
    da1 = scatter_rep(dot(dp, wq, 1, 1))
    input_grad = dm + norm_back(da1 * params[:, 0], n1, r1)
    input_grad = input_grad.astype(BF16).reshape(batch, seq, width)

    def place(piece):
        return lax.dynamic_update_slice_in_dim(jnp.zeros((width,), F32), piece, r * quarter, 0)

    vec = jnp.stack(
        [
            jnp.sum(da1 * n1, axis=0),
            jnp.sum(da1, axis=0),
            place(col[:quarter]),
            place(col[2 * quarter :]),
            jnp.sum(dm, axis=0),
            jnp.sum(da2 * n2, axis=0),
            jnp.sum(da2, axis=0),
            jnp.sum(ef, axis=0),
        ],
        axis=1,
    )
    vec = lax.psum(lax.psum_scatter(vec, "shard", scatter_dimension=0, tiled=True), "rep")
    upb = lax.all_gather(lax.psum(upb, "shard"), "rep", axis=0, tiled=True)

    def columns(g):
        return lax.all_gather(g, "rep", axis=0).transpose(1, 0, 2).astype(F32)

    g_down = columns(g_down).reshape(rows, -1)
    g_up = columns(g_up).reshape(rows, -1)
    g_qkv = columns(g_qkv).reshape(rows, reps, 3, quarter).transpose(0, 2, 1, 3).reshape(rows, -1)
    g_out = lax.psum(g_out, "rep").astype(F32)
    return (outputs, input_grad, g_qkv, g_out, g_up, g_down, vec, upb)


def solution(mesh):
    reps = mesh.shape["rep"]
    token = P(("rep", "shard"), None, None)
    row = P("shard", None)

    def body(*args):
        return per_device(reps, *args)

    return jax.shard_map(
        body,
        mesh=mesh,
        in_specs=(token, token, row, row, row, row, row, P()),
        out_specs=(token, token, row, row, row, row, row, P()),
        check_vma=False,
    )
```

```python
import functools
import math

import jax
import jax.numpy as jnp
from jax import lax
from jax.experimental import pallas as pl
from jax.experimental.pallas import tpu as pltpu
from jax.sharding import PartitionSpec as P

HEAD_DIM = 72
EPSILON = 1e-06
GELU_COEF = 0.044715
ROOT_TWO_PI = math.sqrt(2.0 / math.pi)
SCALE = 1.0 / math.sqrt(HEAD_DIM)
F32 = jnp.float32
BF16 = jnp.bfloat16
RING = 8
HOPS = RING - 1


def dot(a, b, ca=1, cb=0):
    return lax.dot_general(a, b, (((ca,), (cb,)), ((), ())), preferred_element_type=F32)


def ring_row(pos):
    return 2 * pos + (pos // 4) * (15 - 4 * pos)


def mod8(v):
    return lax.rem(v + 4 * RING, RING)


def rows16(start, size):
    return pl.ds(pl.multiple_of(start, 16), size)


def normed(x):
    mean = jnp.mean(x, axis=-1, keepdims=True)
    cen = x - mean
    inv = lax.rsqrt(jnp.mean(cen * cen, axis=-1, keepdims=True) + EPSILON)
    return cen * inv, inv


def norm_back(dn, n, inv):
    a = jnp.mean(dn, axis=-1, keepdims=True)
    b = jnp.mean(dn * n, axis=-1, keepdims=True)
    return inv * (dn - a - n * b)


SCRATCH = dict(
    wb=lambda c: pltpu.VMEM((3, c.d, c.c), BF16),
    wo4=lambda c: pltpu.VMEM((4, c.q, c.qp), BF16),
    wo=lambda c: pltpu.VMEM((c.q, c.d), BF16),
    xa=lambda c: pltpu.VMEM((4, c.t, c.c), BF16),
    ea=lambda c: pltpu.VMEM((4, c.t, c.d), BF16),
    a1=lambda c: pltpu.VMEM((4, c.t, c.d), BF16),
    a2=lambda c: pltpu.VMEM((4, c.t, c.d), BF16),
    dmb=lambda c: pltpu.VMEM((4, c.t, c.d), BF16),
    pq=lambda c: pltpu.VMEM((4, c.t, c.c), BF16),
    oq=lambda c: pltpu.VMEM((4, c.t, c.qp), BF16),
    lse=lambda c: pltpu.VMEM((4, c.t, 128), F32),
    act=lambda c: pltpu.VMEM((4, c.t, c.c), BF16),
    der=lambda c: pltpu.VMEM((4, c.t, c.c), BF16),
    mid=lambda c: pltpu.VMEM((c.t, c.d), F32),
    dm=lambda c: pltpu.VMEM((c.t, c.d), F32),
    do=lambda c: pltpu.VMEM((4, c.t, c.qp), BF16),
    part=lambda c: pltpu.VMEM((4, c.t, c.d), BF16),
    xs=lambda c: pltpu.VMEM((c.t, c.d), BF16),
    cr=lambda c: pltpu.VMEM((2, 2, c.t, c.d), BF16),
    xr=lambda c: pltpu.VMEM((2, c.t, c.d), BF16),
    gd=lambda c: pltpu.VMEM((c.d, c.c), BF16),
    slot=lambda c: pltpu.VMEM((3, HOPS, c.b, c.c), BF16),
    fin=lambda c: pltpu.VMEM((3, 4, c.b, c.c), BF16),
    ogs=lambda c: pltpu.VMEM((4, c.q, c.qp), BF16),
    vb=lambda c: pltpu.VMEM((RING, c.b, 128), BF16),
    vt=lambda c: pltpu.VMEM((16, c.d), F32),
    vg=lambda c: pltpu.VMEM((RING, 8, c.d), F32),
    vf=lambda c: pltpu.VMEM((4, 8, c.d), F32),
    ag_s=lambda c: pltpu.SemaphoreType.DMA((3, 2, 2, HOPS)),
    ag_r=lambda c: pltpu.SemaphoreType.DMA((3, 2, 2, HOPS)),
    rs_s=lambda c: pltpu.SemaphoreType.DMA((3, 2, 2, HOPS)),
    rs_r=lambda c: pltpu.SemaphoreType.DMA((3, 2, 2, HOPS)),
    sm_s=lambda c: pltpu.SemaphoreType.DMA((2, 2, 4)),
    sm_r=lambda c: pltpu.SemaphoreType.DMA((2, 2, 4)),
    ex_s=lambda c: pltpu.SemaphoreType.DMA((8, 3)),
    ex_r=lambda c: pltpu.SemaphoreType.DMA((8, 3)),
    sum_s=lambda c: pltpu.SemaphoreType.DMA((4, 3)),
    sum_r=lambda c: pltpu.SemaphoreType.DMA((4, 3)),
    aa_s=lambda c: pltpu.SemaphoreType.DMA((2, 3)),
    aa_r=lambda c: pltpu.SemaphoreType.DMA((2, 3)),
    out_s=lambda c: pltpu.SemaphoreType.DMA((6,)),
)


class Sizes:
    def __init__(self, d, t, c, b, sub):
        self.d, self.t, self.c, self.b, self.sub = d, t, c, b, sub
        self.q = d // 4
        self.qp = -(-self.q // 128) * 128
        self.heads = self.q // HEAD_DIM


def kernel(c, w_ref, x_ref, e_ref, v_ref, ub_ref, out_ref, ing_ref, g0_ref, g1_ref, g2_ref, vo_ref, *refs):
    z = type("Refs", (), dict(zip(SCRATCH, refs)))
    d, t, nb, q, heads = c.d, c.t, c.b, c.q, c.heads
    r = lax.axis_index("rep")
    shard = lax.axis_index("shard")
    row, sub = shard // c.sub, lax.rem(shard, c.sub)
    za, yb = row // 2, lax.rem(row, 2)
    pos = za + yb * (7 - 2 * za)

    def ring_dev(p):
        return (r, ring_row(mod8(p)) * c.sub + sub)

    ahead = (ring_dev(pos + 1), ring_dev(pos - 1))
    core = r + 1 - 2 * lax.rem(r, 2)
    cross = lax.rem(r + 2, 4)
    diag = lax.rem(core + 2, 4)
    core_dev, cross_dev, diag_dev = (core, shard), (cross, shard), (diag, shard)

    pending = {}

    def rcopy(src, dst, ss, rs, dev):
        return pltpu.make_async_remote_copy(
            src_ref=src, dst_ref=dst, send_sem=ss, recv_sem=rs,
            device_id=dev, device_id_type=pl.DeviceIdType.MESH,
        )

    def send(src, dst, ss, rs, dev):
        cp = rcopy(src, dst, ss, rs, dev)
        cp.start()
        pending[id(cp)] = cp
        return cp

    def settle(cp):
        cp.wait_send()
        del pending[id(cp)]

    barrier = pltpu.get_barrier_semaphore()
    peers = (*ahead, core_dev, cross_dev, diag_dev)
    for dev in peers:
        pl.semaphore_signal(barrier, inc=1, device_id=dev, device_id_type=pl.DeviceIdType.MESH)
    pl.semaphore_wait(barrier, len(peers))

    half = (nb // 2 + 15) // 16 * 16
    bands = ((0, half), (half, nb - half))
    tiles = c.c // 128
    low = (tiles + 1) // 2 * 128

    def cols(k, way):
        cut = low if k % 2 == 0 else c.c - low
        return slice(0, cut) if way == 0 else slice(cut, c.c)

    sign = (1, -1)

    ag_sent = {0: [], 1: [], 2: []}

    def wblock(k, p, h, way):
        start = ring_row(mod8(p)) * nb + bands[h][0]
        return z.wb.at[k, rows16(start, bands[h][1]), cols(k, way)]

    def ag_wait(k, hop):
        for h in range(2):
            for way in range(2):
                dst = wblock(k, pos - sign[way] * (1 + hop), h, way)
                rcopy(dst, dst, z.ag_s.at[k, way, h, hop], z.ag_r.at[k, way, h, hop], ahead[way]).wait_recv()

    def ag(k, hop):
        for h in range(2):
            for way in range(2):
                origin = pos - sign[way] * hop
                dst = wblock(k, origin, h, way)
                if hop == 0:
                    src = w_ref.at[k, pl.ds(bands[h][0], bands[h][1]), cols(k, way)]
                else:
                    src = dst
                    rcopy(
                        dst, dst, z.ag_s.at[k, way, h, hop - 1], z.ag_r.at[k, way, h, hop - 1], ahead[way]
                    ).wait_recv()
                ag_sent[k].append(
                    send(src, dst, z.ag_s.at[k, way, h, hop], z.ag_r.at[k, way, h, hop], ahead[way])
                )

    grads = {}

    def rs(k, hop):
        for h in range(2):
            for way in range(2):
                owner = pos - sign[way] * (1 + hop)
                start = ring_row(mod8(owner)) * nb + bands[h][0]
                mine = grads[k].at[rows16(start, bands[h][1]), cols(k, way)]
                here = lambda i: z.slot.at[k, i, pl.ds(bands[h][0], bands[h][1]), cols(k, way)]
                src = mine
                if hop > 0:
                    src = here(hop - 1)
                    rcopy(
                        src, src, z.rs_s.at[k, way, h, hop - 1], z.rs_r.at[k, way, h, hop - 1], ahead[way]
                    ).wait_recv()
                    src[...] = (src[...].astype(F32) + mine[...].astype(F32)).astype(BF16)
                send(src, here(hop), z.rs_s.at[k, way, h, hop], z.rs_r.at[k, way, h, hop], ahead[way])

    def rs_end(k):
        for h in range(2):
            for way in range(2):
                src = z.slot.at[k, HOPS - 1, pl.ds(bands[h][0], bands[h][1]), cols(k, way)]
                rcopy(
                    src, src, z.rs_s.at[k, way, h, HOPS - 1], z.rs_r.at[k, way, h, HOPS - 1], ahead[way]
                ).wait_recv()
                mine = grads[k].at[rows16(row * nb + bands[h][0], bands[h][1]), cols(k, way)]
                z.fin[k, r, pl.ds(bands[h][0], bands[h][1]), cols(k, way)] = (
                    src[...].astype(F32) + mine[...].astype(F32)
                ).astype(BF16)

    def small(n, buf, hop, own=None):
        for way in range(2):
            if hop < 4 - way:
                if hop > 0:
                    small_wait(n, buf, hop - 1, way)
                blk = buf.at[ring_row(mod8(pos - sign[way] * hop))]
                src = blk if own is None or hop > 0 else own
                send(src, blk, z.sm_s.at[n, way, hop], z.sm_r.at[n, way, hop], ahead[way])

    def small_wait(n, buf, hop, way):
        blk = buf.at[ring_row(mod8(pos - sign[way] * (hop + 1)))]
        rcopy(blk, blk, z.sm_s.at[n, way, hop], z.sm_r.at[n, way, hop], ahead[way]).wait_recv()

    def share(n, buf, own=None):
        dst = buf.at[r]
        own = dst if own is None else own
        return [
            send(own, dst, z.ex_s.at[n, 0], z.ex_r.at[n, 0], cross_dev),
            send(own, dst, z.ex_s.at[n, 1], z.ex_r.at[n, 1], core_dev),
        ]

    def share_wait(n, buf, i):
        blk = buf.at[(cross, core, diag)[i]]
        rcopy(blk, blk, z.ex_s.at[n, i], z.ex_r.at[n, i], (cross_dev, core_dev, core_dev)[i]).wait_recv()

    def share_relay(n, buf):
        share_wait(n, buf, 0)
        blk = buf.at[cross]
        return send(blk, blk, z.ex_s.at[n, 2], z.ex_r.at[n, 2], core_dev)

    def sum_core(n, terms, i):
        image = (diag, core)[i]
        return send(terms.at[image], z.cr.at[n % 2, i], z.sum_s.at[n, i], z.sum_r.at[n, i], core_dev)

    def sum_wait(n, i):
        dst = (z.cr.at[n % 2, 0], z.cr.at[n % 2, 1], z.xr.at[n % 2])[i]
        rcopy(dst, dst, z.sum_s.at[n, i], z.sum_r.at[n, i], (core_dev, core_dev, cross_dev)[i]).wait_recv()

    def sum_cross(n, terms):
        sum_wait(n, 0)
        z.xs[...] = (terms[cross].astype(F32) + z.cr[n % 2, 0].astype(F32)).astype(BF16)
        return send(z.xs, z.xr.at[n % 2], z.sum_s.at[n, 2], z.sum_r.at[n, 2], cross_dev)

    def sum_take(n, terms, sl):
        return (
            terms[r, sl, :].astype(F32) + z.cr[n % 2, 1, sl, :].astype(F32) + z.xr[n % 2, sl, :].astype(F32)
        )

    def tiles_of(total, step, fn):
        def body(j, carry):
            fn(pl.ds(pl.multiple_of(j * step, step), step))
            return carry

        lax.fori_loop(0, total // step, body, 0)

    z.vb[row] = v_ref[...]
    small(0, z.vb, 0, v_ref)
    ag(0, 0)
    z.xa[r] = x_ref[...]
    z.ea[r] = e_ref[...]
    share(0, z.xa, x_ref)
    share(1, z.ea, e_ref)
    for k in range(3):
        z.wb[k, rows16(row * nb, nb), :] = w_ref[k]
    small(0, z.vb, 1)
    ag(0, 1)
    small(0, z.vb, 2)
    ag(0, 2)
    small(0, z.vb, 3)
    small_wait(0, z.vb, 3, 0)
    small_wait(0, z.vb, 2, 1)
    vec = z.vb[...].reshape(d, 128).astype(F32)
    z.vt[...] = jnp.transpose(vec)[0:16, :]
    ag(0, 3)

    def first_norm(i):
        def fn(sl):
            n, _ = normed(z.xa[i, sl, :].astype(F32))
            z.a1[i, sl, :] = (n * z.vt[0:1, :] + z.vt[1:2, :]).astype(BF16)

        tiles_of(t, 64, fn)

    first_norm(r)
    share_wait(0, z.xa, 1)
    first_norm(core)
    ag(0, 4)
    sent_x = share_relay(0, z.xa)
    ag(1, 0)
    first_norm(cross)
    ag(0, 5)
    share_wait(0, z.xa, 2)
    first_norm(diag)
    ag(0, 6)
    share_relay(1, z.ea)
    share_wait(1, z.ea, 1)
    ag(1, 1)
    ag_wait(0, 6)

    def swap(n, src, dst):
        for i, (who, dev) in enumerate(((cross, cross_dev), (diag, diag_dev), (core, core_dev))):
            send(src(who), dst.at[r], z.aa_s.at[n, i], z.aa_r.at[n, i], dev)

    def swap_wait(n, dst):
        for i, (who, dev) in enumerate(((cross, cross_dev), (diag, diag_dev), (core, core_dev))):
            blk = dst.at[who]
            rcopy(blk, blk, z.aa_s.at[n, i], z.aa_r.at[n, i], dev).wait_recv()

    swap(0, lambda who: z.wb.at[0, rows16(who * q, q), 0 : c.qp], z.wo4)
    z.wo4[r] = z.wb[0, rows16(r * q, q), 0 : c.qp]

    def of_rep(line):
        out = z.vt[line : line + 1, 0:q]
        for i in range(1, 4):
            out = jnp.where(r == i, z.vt[line : line + 1, i * q : (i + 1) * q], out)
        return out

    zero = jnp.zeros((1, q), F32)
    bias = jnp.concatenate([zero, of_rep(2), zero, of_rep(3)], axis=1)

    def project(i):
        z.pq[i] = (dot(z.a1[i], z.wb[0]) + bias).astype(BF16)

    def head(i, part, h):
        start = (part + 1) * q + h * HEAD_DIM
        return z.pq[i, :, start : start + HEAD_DIM]

    def attend(i):
        for h in range(heads):
            s = dot(head(i, 0, h), head(i, 1, h), 1, 1) * SCALE
            top = jnp.max(s, axis=-1, keepdims=True)
            ex = jnp.exp(s - top)
            total = jnp.sum(ex, axis=-1, keepdims=True)
            w = (ex * (1.0 / total)).astype(BF16)
            z.oq[i, :, h * HEAD_DIM : (h + 1) * HEAD_DIM] = dot(w, head(i, 2, h)).astype(BF16)
            z.lse[i, :, h : h + 1] = top + jnp.log(total)

    far_first = (diag, cross, core, r)
    near_first = (r, core, cross, diag)

    def pick(order, n):
        out = order[0]
        for i in range(1, 4):
            out = out + (n == i).astype(jnp.int32) * (order[i] - order[0])
        return out

    def in_order(order, fn, lo=0, hi=4):
        def body(n, carry):
            fn(pick(order, n))
            return carry

        lax.fori_loop(lo, hi, body, 0)

    in_order(far_first, project, 0, 2)
    ag(1, 2)
    in_order(far_first, project, 2, 4)
    in_order(far_first, attend, 0, 1)
    ag(1, 3)
    in_order(far_first, attend, 1, 2)
    ag(1, 4)
    in_order(far_first, attend, 2, 3)
    ag(1, 5)
    ag(2, 0)
    in_order(far_first, attend, 3, 4)
    swap_wait(0, z.wo4)
    for i in range(4):
        z.wo[:, i * q : (i + 1) * q] = z.wo4[i, :, 0:q]

    def out_term(i):
        z.part[i] = dot(z.oq[i, :, 0:q], z.wo[...]).astype(BF16)

    in_order(far_first, out_term)
    sent0 = [sum_core(0, z.part, 0), sum_core(0, z.part, 1)]
    ag(1, 6)
    sentx = sum_cross(0, z.part)
    ag(2, 1)
    ag_wait(1, 6)
    ag(2, 2)
    sum_wait(0, 1)
    sum_wait(0, 2)

    def middle(sl):
        m = x_ref[sl, :].astype(F32) + sum_take(0, z.part, sl) + z.vt[4:5, :]
        z.mid[sl, :] = m
        n, _ = normed(m)
        z.a2[r, sl, :] = (n * z.vt[5:6, :] + z.vt[6:7, :]).astype(BF16)

    tiles_of(t, 64, middle)
    share(2, z.a2)

    def up(i):
        u = dot(z.a2[i], z.wb[1]) + ub_ref[...]
        u2 = u * u
        th = jnp.tanh(ROOT_TWO_PI * (u * (1.0 + GELU_COEF * u2)))
        hp = 0.5 * (1.0 + th)
        z.act[i] = (u * hp).astype(BF16)
        z.der[i] = (
            hp + 0.5 * u * (1.0 - th * th) * (ROOT_TWO_PI * (1.0 + 3.0 * GELU_COEF * u2))
        ).astype(BF16)

    ag(2, 3)
    in_order(near_first, up, 0, 1)
    share_wait(2, z.a2, 1)
    ag(2, 4)
    in_order(near_first, up, 1, 2)
    ag(2, 5)
    share_relay(2, z.a2)
    in_order(near_first, up, 2, 3)
    ag(2, 6)
    share_wait(2, z.a2, 2)
    in_order(near_first, up, 3, 4)
    share_wait(1, z.ea, 2)

    def grad_of(dst, left, right):
        def fn(sl):
            acc = dot(left[0, :, sl], right[0], 0, 0)
            for i in range(1, 4):
                acc += dot(left[i, :, sl], right[i], 0, 0)
            dst[sl, :] = acc.astype(BF16)

        return fn

    tiles_of(d, 384, grad_of(z.gd, z.ea, z.act))
    ag_wait(2, 6)
    grads[0] = z.gd
    rs(0, 0)
    for cp in (*sent0, sentx):
        settle(cp)
    z.vg[row] = jnp.zeros((8, d), F32)

    def down_back(i):
        du = dot(z.ea[i], z.wb[2]) * z.der[i].astype(F32)
        z.vg[row, 3:4, :] += jnp.sum(du, axis=0, keepdims=True)
        dub = du.astype(BF16)
        z.der[i] = dub
        z.part[i] = dot(dub, z.wb[1], 1, 1).astype(BF16)

    in_order(far_first, down_back, 0, 1)
    sent1 = [sum_core(1, z.part, 0)]
    in_order(far_first, down_back, 1, 2)
    sentx = sum_cross(1, z.part)
    rs(0, 1)
    in_order(far_first, down_back, 2, 3)
    sent1.append(sum_core(1, z.part, 1))
    in_order(far_first, down_back, 3, 4)
    rs(0, 2)

    def out_back(i):
        z.act[i] = dot(z.act[i], z.wb[2], 1, 1).astype(BF16)

    in_order(far_first, out_back, 0, 2)
    rs(0, 3)
    in_order(far_first, out_back, 2, 4)
    sent2 = [sum_core(2, z.act, 0), sum_core(2, z.act, 1)]
    for cp in ag_sent[2]:
        settle(cp)
    grads[1] = z.wb.at[2]
    up_grad = grad_of(grads[1], z.a2, z.der)
    up_grad(pl.ds(0, 384))
    rs(0, 4)
    up_grad(pl.ds(384, 384))
    sum_wait(1, 1)
    sum_wait(1, 2)

    def second_norm(sl):
        da2 = sum_take(1, z.part, sl)
        e = e_ref[sl, :].astype(F32)
        n, inv = normed(z.mid[sl, :])
        dm = e + norm_back(da2 * z.vt[5:6, :], n, inv)
        z.dm[sl, :] = dm
        z.dmb[r, sl, :] = dm.astype(BF16)
        for line, val in ((4, dm), (5, da2 * n), (6, da2), (7, e)):
            z.vg[row, line : line + 1, :] += jnp.sum(val, axis=0, keepdims=True)

    tiles_of(t, 64, second_norm)
    sent3d = share(3, z.dmb)
    settle(sent_x)
    settle(sentx)
    sentx = sum_cross(2, z.act)
    rs(0, 5)
    up_grad(pl.ds(768, 384))
    rs(1, 0)

    def attend_back(i):
        z.do[i, :, 0:q] = dot(z.dmb[i], z.wo[...], 1, 1).astype(BF16)
        for h in range(heads):
            qh, kh, vh = (head(i, n, h) for n in range(3))
            g = z.do[i, :, h * HEAD_DIM : (h + 1) * HEAD_DIM]
            s = dot(qh, kh, 1, 1) * SCALE
            pr = jnp.exp(s - z.lse[i, :, h : h + 1])
            dv = dot(pr.astype(BF16), g, 0, 0)
            dpr = dot(g, vh, 1, 1)
            delta = jnp.sum(pr * dpr, axis=-1, keepdims=True)
            ds = (pr * (dpr - delta) * SCALE).astype(BF16)
            for n, val in enumerate((dot(ds, kh), dot(ds, qh, 0, 0), dv)):
                start = (n + 1) * q + h * HEAD_DIM
                z.xa[i, :, start : start + HEAD_DIM] = val.astype(BF16)
        z.vg[row, 2:3, :] += jnp.sum(z.xa[i].astype(F32), axis=0, keepdims=True)

    in_order(near_first, attend_back, 0, 1)
    share_wait(3, z.dmb, 1)
    rs(0, 6)
    in_order(near_first, attend_back, 1, 2)
    rs(1, 1)
    share_relay(3, z.dmb)
    rs_end(0)
    share(4, z.fin.at[0])
    in_order(near_first, attend_back, 2, 3)
    rs(1, 2)
    share_wait(3, z.dmb, 2)
    in_order(near_first, attend_back, 3, 4)
    rs(1, 3)

    og = dot(z.oq[0, :, 0:q], z.dmb[0], 0, 0)
    for i in range(1, 4):
        og += dot(z.oq[i, :, 0:q], z.dmb[i], 0, 0)
    for i in range(4):
        z.ogs[i, :, 0:q] = og[:, i * q : (i + 1) * q].astype(BF16)
    swap(1, lambda who: z.ogs.at[who], z.wo4)
    z.wo4[r] = z.ogs[r]
    for cp in ag_sent[1]:
        settle(cp)
    for cp in sent1:
        settle(cp)
    rs(1, 4)

    def first_back(i):
        z.part[i, :, :] = dot(z.xa[i, :, q:], z.wb[0, :, q:], 1, 1).astype(BF16)

    in_order(far_first, first_back, 0, 2)
    sent3 = [sum_core(3, z.part, 0)]
    rs(1, 5)
    in_order(far_first, first_back, 2, 4)
    sent3.append(sum_core(3, z.part, 1))
    sum_wait(2, 1)
    sum_wait(2, 2)

    def last_out(sl):
        z.xs[sl, :] = (z.mid[sl, :] + sum_take(2, z.act, sl) + z.vt[7:8, :]).astype(BF16)

    settle(sentx)
    tiles_of(t, 64, last_out)
    copies = []

    def put(n, src, dst):
        cp = pltpu.make_async_copy(src, dst, z.out_s.at[n])
        cp.start()
        copies.append(cp)
        return cp

    put(0, z.xs, out_ref).wait()
    copies.pop()
    sentx = sum_cross(3, z.part)
    grads[2] = z.wb.at[1]
    tiles_of(d, 384, grad_of(grads[2], z.a1, z.xa))
    swap_wait(1, z.wo4)
    for i in range(4):
        grads[2][i * q : (i + 1) * q, 0:q] = z.wo4[i, :, 0:q]
    rs(1, 6)
    rs(2, 0)
    share_relay(4, z.fin.at[0])
    rs_end(1)
    share(5, z.fin.at[1])
    rs(2, 1)
    sum_wait(3, 1)
    sum_wait(3, 2)

    def last_norm(sl):
        da1 = sum_take(3, z.part, sl)
        n, inv = normed(x_ref[sl, :].astype(F32))
        z.dmb[r, sl, :] = (z.dm[sl, :] + norm_back(da1 * z.vt[0:1, :], n, inv)).astype(BF16)
        for line, val in ((0, da1 * n), (1, da1)):
            z.vg[row, line : line + 1, :] += jnp.sum(val, axis=0, keepdims=True)

    for cp in sent3d:
        settle(cp)
    tiles_of(t, 64, last_norm)
    put(1, z.dmb.at[r], ing_ref)
    small(1, z.vg, 0)
    rs(2, 2)
    small(1, z.vg, 1)
    rs(2, 3)
    small(1, z.vg, 2)
    share_relay(5, z.fin.at[1])
    rs(2, 4)
    small(1, z.vg, 3)
    rs(2, 5)
    small_wait(1, z.vg, 3, 0)
    small_wait(1, z.vg, 2, 1)
    total = z.vg[0]
    for i in range(1, RING):
        total += z.vg[i]
    z.vf[r] = total
    share(7, z.vf)
    rs(2, 6)
    for k in range(2):
        share_wait(4 + k, z.fin.at[k], 1)
        share_wait(4 + k, z.fin.at[k], 2)
        put(2 + k, z.fin.at[k], (g0_ref, g1_ref)[k])
    share_relay(7, z.vf)
    share_wait(7, z.vf, 1)
    share_wait(7, z.vf, 2)
    put(5, z.vf, vo_ref)
    rs_end(2)
    share(6, z.fin.at[2])
    share_relay(6, z.fin.at[2])
    share_wait(6, z.fin.at[2], 1)
    share_wait(6, z.fin.at[2], 2)
    put(4, z.fin.at[2], g2_ref)
    for cp in list(pending.values()):
        settle(cp)
    for cp in copies:
        cp.wait()


def per_device(reps, shards, images, cotangent, w_qkv, w_out, w_up, w_down, vectors, up_bias):
    r = lax.axis_index("rep")
    batch, seq, d = images.shape
    q = d // reps
    hidden = w_up.shape[1]
    ffq = hidden // reps
    wide = -(-max(4 * q, ffq) // 128) * 128
    sub = shards // RING
    groups = [[i * sub + j for j in range(sub)] for i in range(RING)]
    shard = lax.axis_index("shard")

    def take(w, start, size):
        return lax.dynamic_slice_in_dim(w, start, size, 1)

    first = [take(w_out, r * q, q)] + [take(w_qkv, k * d + r * q, q) for k in range(3)]
    pad = ((0, 0), (0, wide - ffq))
    w = jnp.stack(
        [
            jnp.concatenate(first, axis=1),
            jnp.pad(take(w_up, r * ffq, ffq), pad),
            jnp.pad(take(w_down, r * ffq, ffq), pad),
        ]
    )
    v = jnp.pad(vectors, ((0, 0), (0, 128 - vectors.shape[1])))
    if sub > 1:
        w = lax.all_gather(w, "shard", axis=1, tiled=True, axis_index_groups=groups)
        v = lax.all_gather(v, "shard", axis=0, tiled=True, axis_index_groups=groups)
    ub = lax.dynamic_slice_in_dim(up_bias, r * ffq, ffq, 0).astype(F32)
    ub = jnp.pad(ub, (0, wide - ffq)).reshape(1, wide)
    c = Sizes(d, seq, wide, w.shape[1], sub)
    vmem = pl.BlockSpec(memory_space=pltpu.VMEM)
    hbm = pl.BlockSpec(memory_space=pl.ANY)
    grad = jax.ShapeDtypeStruct((4, c.b, wide), BF16)
    tok = jax.ShapeDtypeStruct((seq, d), BF16)
    outputs, input_grad, g_down, g_up, g_first, vf = pl.pallas_call(
        functools.partial(kernel, c),
        out_shape=(tok, tok, grad, grad, grad, jax.ShapeDtypeStruct((4, 8, d), F32)),
        in_specs=[vmem] * 5,
        out_specs=(hbm,) * 6,
        scratch_shapes=[make(c) for make in SCRATCH.values()],
        compiler_params=pltpu.CompilerParams(
            collective_id=0, has_side_effects=True, vmem_limit_bytes=67043328
        ),
    )(w, images.reshape(seq, d), cotangent.reshape(seq, d), v, ub)

    def finish(g):
        g = g.astype(F32)
        if sub > 1:
            g = lax.psum_scatter(g, "shard", scatter_dimension=1, tiled=True, axis_index_groups=groups)
        return g

    def columns(g):
        return jnp.concatenate([g[i, :, :ffq] for i in range(reps)], axis=1)

    g_down, g_up, g_first = finish(g_down), finish(g_up), finish(g_first)
    g_out = jnp.concatenate([g_first[i, :, :q] for i in range(reps)], axis=1)
    g_qkv = jnp.concatenate(
        [g_first[i, :, k * q : (k + 1) * q] for k in range(1, 4) for i in range(reps)], axis=1
    )
    if sub > 1:
        vf = lax.psum(vf, "shard", axis_index_groups=groups)
    whole = jnp.sum(vf, axis=0)
    bias = [jnp.concatenate([vf[i, 2, k * q : (k + 1) * q] for i in range(reps)]) for k in (1, 3)]
    upb = jnp.concatenate([vf[i, 3, :ffq] for i in range(reps)])
    lines = jnp.stack([whole[0], whole[1], *bias, whole[4], whole[5], whole[6], whole[7]], axis=1)
    own = d // shards
    vec = lax.dynamic_slice_in_dim(lines, shard * own, own, 0)
    shape = (batch, seq, d)
    return (
        outputs.reshape(shape),
        input_grad.reshape(shape),
        g_qkv,
        g_out,
        columns(g_up),
        columns(g_down),
        vec,
        upb,
    )


def solution(mesh):
    reps, shards = mesh.shape["rep"], mesh.shape["shard"]
    token = P(("rep", "shard"), None, None)
    line = P("shard", None)

    def body(*args):
        return per_device(reps, shards, *args)

    return jax.shard_map(
        body,
        mesh=mesh,
        in_specs=(token, token, line, line, line, line, line, P()),
        out_specs=(token, token, line, line, line, line, line, P()),
        check_vma=False,
    )
```

```python
import functools
import math

import jax
import jax.numpy as jnp
from jax import lax
from jax.experimental import pallas as pl
from jax.experimental.pallas import tpu as pltpu
from jax.sharding import PartitionSpec as P

HEAD_DIM = 72
EPSILON = 1e-06
GELU_COEF = 0.044715
ROOT_TWO_PI = math.sqrt(2.0 / math.pi)
SCALE = 1.0 / math.sqrt(HEAD_DIM)
F32 = jnp.float32
BF16 = jnp.bfloat16
RING = 8
HOPS = RING - 1
BANDS = 3


def dot(a, b, ca=1, cb=0):
    return lax.dot_general(a, b, (((ca,), (cb,)), ((), ())), preferred_element_type=F32)


def ring_row(pos):
    return 2 * pos + (pos // 4) * (15 - 4 * pos)


def mod8(v):
    return lax.rem(v + 4 * RING, RING)


def rows16(start, size):
    return pl.ds(pl.multiple_of(start, 16), size)


def normed(x):
    mean = jnp.mean(x, axis=-1, keepdims=True)
    cen = x - mean
    inv = lax.rsqrt(jnp.mean(cen * cen, axis=-1, keepdims=True) + EPSILON)
    return cen * inv, inv


def norm_back(dn, n, inv):
    a = jnp.mean(dn, axis=-1, keepdims=True)
    b = jnp.mean(dn * n, axis=-1, keepdims=True)
    return inv * (dn - a - n * b)


SCRATCH = dict(
    raw=lambda c: pltpu.VMEM((2, c.b, c.hidden), BF16),
    wb=lambda c: pltpu.VMEM((3, c.d, c.c), BF16),
    wo4=lambda c: pltpu.VMEM((4, c.q, c.qp), BF16),
    wo=lambda c: pltpu.VMEM((c.q, c.d), BF16),
    xa=lambda c: pltpu.VMEM((4, c.t, c.c), BF16),
    ea=lambda c: pltpu.VMEM((4, c.t, c.d), BF16),
    a1=lambda c: pltpu.VMEM((4, c.t, c.d), BF16),
    a2=lambda c: pltpu.VMEM((4, c.t, c.d), BF16),
    dmb=lambda c: pltpu.VMEM((4, c.t, c.d), BF16),
    pq=lambda c: pltpu.VMEM((4, c.t, c.c), BF16),
    oq=lambda c: pltpu.VMEM((4, c.t, c.qp), BF16),
    lse=lambda c: pltpu.VMEM((4, c.t, 128), F32),
    act=lambda c: pltpu.VMEM((4, c.t, c.c), BF16),
    der=lambda c: pltpu.VMEM((4, c.t, c.c), BF16),
    mid=lambda c: pltpu.VMEM((c.t, c.d), F32),
    dm=lambda c: pltpu.VMEM((c.t, c.d), F32),
    do=lambda c: pltpu.VMEM((c.t, c.qp), BF16),
    part=lambda c: pltpu.VMEM((4, c.t, c.d), BF16),
    xs=lambda c: pltpu.VMEM((2, c.t, c.d), BF16),
    cr=lambda c: pltpu.VMEM((2, 2, c.t, c.d), BF16),
    xr=lambda c: pltpu.VMEM((2, c.t, c.d), BF16),
    gd=lambda c: pltpu.VMEM((c.d, c.c), BF16),
    slot=lambda c: pltpu.VMEM((3, HOPS, c.b, c.c), BF16),
    fin=lambda c: pltpu.VMEM((3, 4, c.b, c.c), BF16),
    ogs=lambda c: pltpu.VMEM((4, c.q, c.qp), BF16),
    vb=lambda c: pltpu.VMEM((RING, 8, c.b), F32),
    vt=lambda c: pltpu.VMEM((8, c.d), F32),
    ub=lambda c: pltpu.VMEM((8, c.c), F32),
    vg=lambda c: pltpu.VMEM((RING, 8, c.d), F32),
    vf=lambda c: pltpu.VMEM((4, 8, c.d), F32),
    ag_s=lambda c: pltpu.SemaphoreType.DMA((3, 2, BANDS, HOPS)),
    ag_r=lambda c: pltpu.SemaphoreType.DMA((3, 2, BANDS, HOPS)),
    rs_s=lambda c: pltpu.SemaphoreType.DMA((3, 2, BANDS, HOPS)),
    rs_r=lambda c: pltpu.SemaphoreType.DMA((3, 2, BANDS, HOPS)),
    sm_s=lambda c: pltpu.SemaphoreType.DMA((2, 2, 4)),
    sm_r=lambda c: pltpu.SemaphoreType.DMA((2, 2, 4)),
    ex_s=lambda c: pltpu.SemaphoreType.DMA((10, 3)),
    ex_r=lambda c: pltpu.SemaphoreType.DMA((10, 3)),
    sum_s=lambda c: pltpu.SemaphoreType.DMA((4, 3)),
    sum_r=lambda c: pltpu.SemaphoreType.DMA((4, 3)),
    aa_s=lambda c: pltpu.SemaphoreType.DMA((2, 3)),
    aa_r=lambda c: pltpu.SemaphoreType.DMA((2, 3)),
    in_s=lambda c: pltpu.SemaphoreType.DMA((6,)),
    out_s=lambda c: pltpu.SemaphoreType.DMA((6,)),
)


class Sizes:
    def __init__(self, d, t, c, b, sub, hidden):
        self.d, self.t, self.c, self.b, self.sub, self.hidden = d, t, c, b, sub, hidden
        self.q = d // 4
        self.f = hidden // 4
        self.qp = -(-self.q // 128) * 128
        self.heads = self.q // HEAD_DIM


def kernel(
    c, wq_ref, wo_ref, wu_ref, wd_ref, x_ref, e_ref, v_ref, ub_ref,
    out_ref, ing_ref, g0_ref, g1_ref, g2_ref, vo_ref, *refs
):
    z = type("Refs", (), dict(zip(SCRATCH, refs)))
    d, t, nb, q, heads = c.d, c.t, c.b, c.q, c.heads
    band = nb // BANDS
    r = lax.axis_index("rep")
    shard = lax.axis_index("shard")
    row, sub = shard // c.sub, lax.rem(shard, c.sub)
    za, yb = row // 2, lax.rem(row, 2)
    pos = za + yb * (7 - 2 * za)

    def ring_dev(p):
        return (r, ring_row(mod8(p)) * c.sub + sub)

    ahead = (ring_dev(pos + 1), ring_dev(pos - 1))
    core = r + 1 - 2 * lax.rem(r, 2)
    cross = lax.rem(r + 2, 4)
    diag = lax.rem(core + 2, 4)
    core_dev, cross_dev, diag_dev = (core, shard), (cross, shard), (diag, shard)
    sign = (1, -1)

    def rcopy(src, dst, kind, index, dev):
        return pltpu.make_async_remote_copy(
            src_ref=src, dst_ref=dst,
            send_sem=getattr(z, kind + "_s").at[index], recv_sem=getattr(z, kind + "_r").at[index],
            device_id=dev, device_id_type=pl.DeviceIdType.MESH,
        )

    def send(src, dst, kind, index, dev):
        rcopy(src, dst, kind, index, dev).start()

    def recv(dst, kind, index, dev):
        rcopy(dst, dst, kind, index, dev).wait_recv()

    def sent(src, kind, index, dev):
        rcopy(src, src, kind, index, dev).wait_send()

    def repeat(count, fn, lo=0):
        def body(n, carry):
            fn(n)
            return carry

        lax.fori_loop(lo, count, body, 0)

    def tiles_of(total, step, fn):
        repeat(total // step, lambda j: fn(pl.ds(pl.multiple_of(j * step, step), step)))

    low = (c.c // 128 + 1) // 2 * 128

    def cols(k, way):
        cut = low if k % 2 == 0 else c.c - low
        return slice(0, cut) if way == 0 else slice(cut, c.c)

    def wblock(k, p, h, way):
        return z.wb.at[k, rows16(ring_row(mod8(p)) * nb + h * band, band), cols(k, way)]

    def ag(k, hop):
        def one(h):
            for way in range(2):
                blk = wblock(k, pos - sign[way] * hop, h, way)
                if not (isinstance(hop, int) and hop == 0):
                    recv(blk, "ag", (k, way, h, hop - 1), ahead[way])
                send(blk, blk, "ag", (k, way, h, hop), ahead[way])

        repeat(BANDS, one)

    def ag_wait(k):
        def one(h):
            for way in range(2):
                recv(wblock(k, pos - sign[way] * RING, h, way), "ag", (k, way, h, HOPS - 1), ahead[way])

        repeat(BANDS, one)

    def ag_sent(k):
        def one(n):
            for way in range(2):
                sent(wblock(k, pos, n // HOPS, way), "ag", (k, way, n // HOPS, lax.rem(n, HOPS)), ahead[way])

        repeat(BANDS * HOPS, one)

    grads = {0: z.gd, 1: z.wb.at[2], 2: z.wb.at[1]}

    def slot(k, hop, h, way):
        return z.slot.at[k, hop, rows16(h * band, band), cols(k, way)]

    def term(k, p, h, way):
        return grads[k].at[rows16(ring_row(mod8(p)) * nb + h * band, band), cols(k, way)]

    def rs(k, hop):
        def one(h):
            for way in range(2):
                src = mine = term(k, pos - sign[way] * (1 + hop), h, way)
                if not (isinstance(hop, int) and hop == 0):
                    src = slot(k, hop - 1, h, way)
                    recv(src, "rs", (k, way, h, hop - 1), ahead[way])
                    src[...] = (src[...].astype(F32) + mine[...].astype(F32)).astype(BF16)
                send(src, slot(k, hop, h, way), "rs", (k, way, h, hop), ahead[way])

        repeat(BANDS, one)

    def rs_end(k, h):
        for way in range(2):
            src = slot(k, HOPS - 1, h, way)
            recv(src, "rs", (k, way, h, HOPS - 1), ahead[way])
            z.fin[k, r, rows16(h * band, band), cols(k, way)] = (
                src[...].astype(F32) + term(k, pos, h, way)[...].astype(F32)
            ).astype(BF16)

    def rs_sent(k):
        def one(n):
            for way in range(2):
                sent(slot(k, 0, n // HOPS, way), "rs", (k, way, n // HOPS, lax.rem(n, HOPS)), ahead[way])

        repeat(BANDS * HOPS, one)

    def small(n, buf, hop):
        for way in range(2):
            if hop < 4 - way:
                if hop > 0:
                    small_wait(n, buf, hop - 1, way)
                blk = buf.at[ring_row(mod8(pos - sign[way] * hop))]
                send(blk, blk, "sm", (n, way, hop), ahead[way])

    def small_wait(n, buf, hop, way):
        recv(buf.at[ring_row(mod8(pos - sign[way] * (hop + 1)))], "sm", (n, way, hop), ahead[way])

    def small_sent(n, buf):
        for way in range(2):
            for hop in range(4 - way):
                sent(buf.at[row], "sm", (n, way, hop), ahead[way])

    ex_dev = (cross_dev, core_dev, core_dev)

    def share(n, at, own=None):
        for i in range(2):
            send(at(r) if own is None else own, at(r), "ex", (n, i), ex_dev[i])

    def share_wait(n, at, i):
        recv(at((cross, core, diag)[i]), "ex", (n, i), ex_dev[i])

    def share_relay(n, at):
        share_wait(n, at, 0)
        send(at(cross), at(cross), "ex", (n, 2), core_dev)

    def share_sent(n, at):
        for i in range(3):
            sent(at(r), "ex", (n, i), ex_dev[i])

    def image_of(buf):
        return lambda i: buf.at[i]

    sum_dev = (core_dev, core_dev, cross_dev)

    def sum_core(n, terms, i):
        send(terms.at[(diag, core)[i]], z.cr.at[n % 2, i], "sum", (n, i), core_dev)

    def sum_wait(n, i):
        recv((z.cr.at[n % 2, 0], z.cr.at[n % 2, 1], z.xr.at[n % 2])[i], "sum", (n, i), sum_dev[i])

    def sum_cross(n, terms):
        sum_wait(n, 0)

        def add(sl):
            z.xs[n % 2, sl, :] = (
                terms[cross, sl, :].astype(F32) + z.cr[n % 2, 0, sl, :].astype(F32)
            ).astype(BF16)

        tiles_of(t, 64, add)
        send(z.xs.at[n % 2], z.xr.at[n % 2], "sum", (n, 2), cross_dev)

    def sum_take(n, terms, sl):
        return (
            terms[r, sl, :].astype(F32) + z.cr[n % 2, 1, sl, :].astype(F32) + z.xr[n % 2, sl, :].astype(F32)
        )

    def sum_sent(n):
        for i in range(3):
            sent(z.xr.at[0], "sum", (n, i), sum_dev[i])

    aa = ((cross, cross_dev), (diag, diag_dev), (core, core_dev))

    def swap(n, src):
        for i, (who, dev) in enumerate(aa):
            send(src(who), z.wo4.at[r], "aa", (n, i), dev)

    def swap_wait(n):
        for i, (who, dev) in enumerate(aa):
            recv(z.wo4.at[who], "aa", (n, i), dev)

    def swap_sent(n):
        for i, (who, dev) in enumerate(aa):
            sent(z.wo4.at[r], "aa", (n, i), dev)

    far_first = (diag, cross, core, r)
    near_first = (r, core, cross, diag)

    def pick(order, n):
        out = order[0]
        for i in range(1, 4):
            out = out + (n == i).astype(jnp.int32) * (order[i] - order[0])
        return out

    loads = [pltpu.make_async_copy(wo_ref, z.slot.at[0, 3], z.in_s.at[3])]
    for k in range(3):
        loads.append(pltpu.make_async_copy(wq_ref.at[:, k * d : (k + 1) * d], z.slot.at[0, k], z.in_s.at[k]))
    for k, ref in enumerate((wu_ref, wd_ref)):
        loads.append(pltpu.make_async_copy(ref, z.raw.at[k], z.in_s.at[4 + k]))
    for cp in loads:
        cp.start()
    z.vb[row] = v_ref[...].astype(F32)
    z.xa[r] = x_ref[...]
    z.ea[r] = e_ref[...]
    barrier = pltpu.get_barrier_semaphore()
    peers = (*ahead, core_dev, cross_dev, diag_dev)
    for dev in peers:
        pl.semaphore_signal(barrier, inc=1, device_id=dev, device_id_type=pl.DeviceIdType.MESH)
    pl.semaphore_wait(barrier, len(peers))
    xa, ea, a2s, dms = (image_of(b) for b in (z.xa, z.ea, z.a2, z.dmb))
    share(0, xa, x_ref)
    small(0, z.vb, 0)
    share(1, ea, e_ref)
    own = rows16(row * nb, nb)
    for cp in loads[:4]:
        cp.wait()
    for i in range(4):

        @pl.when(r == i)
        def _():
            for k in range(4):
                z.wb[0, own, k * q : (k + 1) * q] = z.slot[0, (k + 3) % 4, :, i * q : (i + 1) * q]

    ag(0, 0)
    for cp in loads[4:]:
        cp.wait()
    z.ub[...] = jnp.zeros_like(z.ub)
    for i in range(4):

        @pl.when(r == i)
        def _():
            for k in range(2):
                z.wb[1 + k, own, 0 : c.f] = z.raw[k, :, i * c.f : (i + 1) * c.f]
            z.ub[0:1, 0 : c.f] = ub_ref[0:1, i * c.f : (i + 1) * c.f].astype(F32)

    for k in range(2):
        z.wb[1 + k, own, c.f :] = jnp.zeros((nb, c.c - c.f), BF16)

    small(0, z.vb, 1)
    ag(0, 1)
    small(0, z.vb, 2)
    ag(0, 2)
    small(0, z.vb, 3)
    small_wait(0, z.vb, 3, 0)
    small_wait(0, z.vb, 2, 1)
    for s in range(RING):
        z.vt[:, s * nb : (s + 1) * nb] = z.vb[s]
    ag(0, 3)

    def first_norm(i):
        def fn(sl):
            n, _ = normed(z.xa[i, sl, :].astype(F32))
            z.a1[i, sl, :] = (n * z.vt[0:1, :] + z.vt[1:2, :]).astype(BF16)

        tiles_of(t, 64, fn)

    first_norm(r)
    share_wait(0, xa, 1)
    first_norm(core)
    ag(0, 4)
    share_relay(0, xa)
    first_norm(cross)
    ag(0, 5)
    share_wait(0, xa, 2)
    ag(1, 0)
    first_norm(diag)
    ag(0, 6)
    ag(2, 0)
    ag_wait(0)
    swap(0, lambda who: z.wb.at[0, rows16(who * q, q), 0 : c.qp])
    z.wo4[r] = z.wb[0, rows16(r * q, q), 0 : c.qp]

    def of_rep(line):
        out = z.vt[line : line + 1, 0:q]
        for i in range(1, 4):
            out = jnp.where(r == i, z.vt[line : line + 1, i * q : (i + 1) * q], out)
        return out

    z.ub[1:2, :] = jnp.zeros((1, c.c), F32)
    z.ub[1:2, q : 2 * q] = of_rep(2)
    z.ub[1:2, 3 * q : 4 * q] = of_rep(3)

    def head(i, part, h):
        start = (part + 1) * q + h * HEAD_DIM
        return z.pq[i, :, start : start + HEAD_DIM]

    def attention(n):
        i = pick(far_first, n)
        z.pq[i] = (dot(z.a1[i], z.wb[0]) + z.ub[1:2, :]).astype(BF16)
        ag(1, n + 1)
        for h in range(heads):
            s = dot(head(i, 0, h), head(i, 1, h), 1, 1) * SCALE
            top = jnp.max(s, axis=-1, keepdims=True)
            ex = jnp.exp(s - top)
            total = jnp.sum(ex, axis=-1, keepdims=True)
            w = (ex * (1.0 / total)).astype(BF16)
            z.oq[i, :, h * HEAD_DIM : (h + 1) * HEAD_DIM] = dot(w, head(i, 2, h)).astype(BF16)
            z.lse[i, :, h : h + 1] = top + jnp.log(total)

    repeat(4, attention)
    share_relay(1, ea)
    swap_wait(0)
    for i in range(4):
        z.wo[:, i * q : (i + 1) * q] = z.wo4[i, :, 0:q]

    def out_term(n):
        i = pick(far_first, n)
        z.part[i] = dot(z.oq[i, :, 0:q], z.wo[...]).astype(BF16)
        pl.when(n == 0)(lambda: sum_core(0, z.part, 0))
        pl.when(n == 1)(lambda: sum_cross(0, z.part))
        pl.when(n == 2)(lambda: sum_core(0, z.part, 1))

    repeat(4, out_term)
    ag(1, 5)
    ag(2, 1)
    ag(1, 6)
    ag(2, 2)
    sum_wait(0, 1)
    sum_wait(0, 2)

    def middle(sl):
        m = x_ref[sl, :].astype(F32) + sum_take(0, z.part, sl) + z.vt[4:5, :]
        z.mid[sl, :] = m
        n, _ = normed(m)
        z.a2[r, sl, :] = (n * z.vt[5:6, :] + z.vt[6:7, :]).astype(BF16)

    tiles_of(t, 64, middle)
    share(2, a2s)
    ag_wait(1)

    def up(n):
        i = pick(near_first, n)
        ag(2, n + 3)
        pl.when(n == 1)(lambda: share_wait(2, a2s, 1))
        pl.when(n == 2)(lambda: share_relay(2, a2s))
        pl.when(n == 3)(lambda: share_wait(2, a2s, 2))
        u = dot(z.a2[i], z.wb[1]) + z.ub[0:1, :]
        u2 = u * u
        th = jnp.tanh(ROOT_TWO_PI * (u * (1.0 + GELU_COEF * u2)))
        hp = 0.5 * (1.0 + th)
        z.act[i] = (u * hp).astype(BF16)
        z.der[i] = (
            hp + 0.5 * u * (1.0 - th * th) * (ROOT_TWO_PI * (1.0 + 3.0 * GELU_COEF * u2))
        ).astype(BF16)

    repeat(4, up)
    share_wait(1, ea, 1)
    share_wait(1, ea, 2)

    def grad_of(dst, left, right):
        def fn(sl):
            acc = dot(left[0, :, sl], right[0], 0, 0)
            for i in range(1, 4):
                acc += dot(left[i, :, sl], right[i], 0, 0)
            dst[sl, :] = acc.astype(BF16)

        return fn

    tiles_of(d, 384, grad_of(grads[0], z.ea, z.act))
    rs(0, 0)
    ag_wait(2)
    sum_sent(0)
    z.vg[row] = jnp.zeros((8, d), F32)

    def down_back(n):
        i = pick(far_first, n)
        du = dot(z.ea[i], z.wb[2]) * z.der[i].astype(F32)
        z.vg[row, 3:4, :] += jnp.sum(du, axis=0, keepdims=True)
        dub = du.astype(BF16)
        z.der[i] = dub
        z.part[i] = dot(dub, z.wb[1], 1, 1).astype(BF16)
        pl.when(n == 0)(lambda: sum_core(1, z.part, 0))
        pl.when(n == 1)(lambda: sum_cross(1, z.part))
        pl.when(n == 2)(lambda: sum_core(1, z.part, 1))
        pl.when(n >= 1)(lambda: rs(0, n))

    repeat(4, down_back)

    def out_back(n):
        z.act[n] = dot(z.act[n], z.wb[2], 1, 1).astype(BF16)

    repeat(4, out_back)
    rs(0, 4)
    sum_core(2, z.act, 0)
    sum_core(2, z.act, 1)
    ag_sent(2)

    def up_grad(n):
        grad_of(grads[1], z.a2, z.der)(pl.ds(pl.multiple_of(n * 384, 384), 384))
        pl.when(n == 1)(lambda: rs(0, 5))

    repeat(d // 384, up_grad)
    rs(1, 0)
    sum_wait(1, 1)
    sum_wait(1, 2)

    def second_norm(sl):
        da2 = sum_take(1, z.part, sl)
        e = e_ref[sl, :].astype(F32)
        n, inv = normed(z.mid[sl, :])
        dm = e + norm_back(da2 * z.vt[5:6, :], n, inv)
        z.dm[sl, :] = dm
        z.dmb[r, sl, :] = dm.astype(BF16)
        for line, val in ((4, dm), (5, da2 * n), (6, da2), (7, e)):
            z.vg[row, line : line + 1, :] += jnp.sum(val, axis=0, keepdims=True)

    tiles_of(t, 64, second_norm)
    share(3, dms)
    share_sent(0, xa)

    def fins(k, h=None):
        rows = slice(0, nb) if h is None else slice(h * band, (h + 1) * band)
        return lambda i: z.fin.at[k, i, rows]

    def far_ready():
        for h in range(BANDS):
            rs_end(0, h)
        share_relay(3, dms)
        share_wait(3, dms, 2)
        og = dot(z.oq[0, :, 0:q], z.dmb[0], 0, 0)
        for i in range(1, 4):
            og += dot(z.oq[i, :, 0:q], z.dmb[i], 0, 0)
        for i in range(4):
            z.ogs[i, :, 0:q] = og[:, i * q : (i + 1) * q].astype(BF16)
        swap(1, lambda who: z.ogs.at[who])
        z.wo4[r] = z.ogs[r]
        share(4, fins(0))

    def attend_back(n):
        i = pick(near_first, n)
        pl.when(n == 1)(lambda: share_wait(3, dms, 1))
        pl.when(n == 2)(far_ready)
        z.do[:, 0:q] = dot(z.dmb[i], z.wo[...], 1, 1).astype(BF16)
        for h in range(heads):
            qh, kh, vh = (head(i, m, h) for m in range(3))
            g = z.do[:, h * HEAD_DIM : (h + 1) * HEAD_DIM]
            s = dot(qh, kh, 1, 1) * SCALE
            pr = jnp.exp(s - z.lse[i, :, h : h + 1])
            dv = dot(pr.astype(BF16), g, 0, 0)
            dpr = dot(g, vh, 1, 1)
            delta = jnp.sum(pr * dpr, axis=-1, keepdims=True)
            ds = (pr * (dpr - delta) * SCALE).astype(BF16)
            for m, val in enumerate((dot(ds, kh), dot(ds, qh, 0, 0), dv)):
                start = (m + 1) * q + h * HEAD_DIM
                z.xa[i, :, start : start + HEAD_DIM] = val.astype(BF16)
        z.vg[row, 2:3, :] += jnp.sum(z.xa[i].astype(F32), axis=0, keepdims=True)
        pl.when(n == 0)(lambda: rs(0, 6))
        rs(1, n + 1)

    repeat(4, attend_back)
    ag_sent(1)
    sum_sent(1)

    def first_grad(n):
        grad_of(grads[2], z.a1, z.xa)(pl.ds(pl.multiple_of(n * 384, 384), 384))
        pl.when(n == 1)(lambda: rs(1, 5))

    repeat(d // 384, first_grad)
    swap_wait(1)
    for i in range(4):
        grads[2][i * q : (i + 1) * q, 0:q] = z.wo4[i, :, 0:q]
    rs(2, 0)
    rs(1, 6)

    def first_back(n):
        i = pick(far_first, n)
        z.part[i] = dot(z.xa[i, :, q:], z.wb[0, :, q:], 1, 1).astype(BF16)
        pl.when(n == 0)(lambda: sum_core(3, z.part, 0))
        pl.when(n == 1)(lambda: sum_cross(3, z.part))
        pl.when(n == 2)(lambda: sum_core(3, z.part, 1))

    repeat(4, first_back)
    rs(2, 1)
    for h in range(BANDS):
        rs_end(1, h)
    sum_cross(2, z.act)
    share(5, fins(1))
    share_relay(4, fins(0))
    rs(2, 2)
    copies = []

    def put(n, src, dst):
        cp = pltpu.make_async_copy(src, dst, z.out_s.at[n])
        cp.start()
        copies.append(cp)

    for i in (1, 2):
        share_wait(4, fins(0), i)
    put(2, z.fin.at[0], g0_ref)
    rs(2, 3)
    sum_wait(3, 1)
    sum_wait(3, 2)
    share_sent(3, dms)

    def last_norm(sl):
        da1 = sum_take(3, z.part, sl)
        n, inv = normed(x_ref[sl, :].astype(F32))
        z.dmb[r, sl, :] = (z.dm[sl, :] + norm_back(da1 * z.vt[0:1, :], n, inv)).astype(BF16)
        for line, val in ((0, da1 * n), (1, da1)):
            z.vg[row, line : line + 1, :] += jnp.sum(val, axis=0, keepdims=True)

    tiles_of(t, 64, last_norm)
    put(1, z.dmb.at[r], ing_ref)
    small(1, z.vg, 0)
    rs(2, 4)
    small(1, z.vg, 1)
    sum_wait(2, 1)
    sum_wait(2, 2)
    share_sent(2, a2s)

    def last_out(sl):
        z.a2[r, sl, :] = (z.mid[sl, :] + sum_take(2, z.act, sl) + z.vt[7:8, :]).astype(BF16)

    tiles_of(t, 64, last_out)
    put(0, z.a2.at[r], out_ref)
    small(1, z.vg, 2)
    rs(2, 5)
    small(1, z.vg, 3)
    share_relay(5, fins(1))
    small_wait(1, z.vg, 3, 0)
    small_wait(1, z.vg, 2, 1)
    total = z.vg[0]
    for i in range(1, RING):
        total += z.vg[i]
    z.vf[r] = total
    vfs = image_of(z.vf)
    share(6, vfs)
    rs(2, 6)
    for i in (1, 2):
        share_wait(5, fins(1), i)
    put(3, z.fin.at[1], g1_ref)
    for h in range(BANDS):
        rs_end(2, h)
        share(7 + h, fins(2, h))
    share_relay(6, vfs)
    for h in range(BANDS):
        share_relay(7 + h, fins(2, h))
    for i in (1, 2):
        share_wait(6, vfs, i)
    put(5, z.vf, vo_ref)
    for h in range(BANDS):
        for i in (1, 2):
            share_wait(7 + h, fins(2, h), i)
    put(4, z.fin.at[2], g2_ref)
    ag_sent(0)
    for k in range(3):
        rs_sent(k)
    for n, buf in enumerate((z.vb, z.vg)):
        small_sent(n, buf)
        swap_sent(n)
    share_sent(1, ea)
    share_sent(4, fins(0))
    share_sent(5, fins(1))
    share_sent(6, vfs)
    for h in range(BANDS):
        share_sent(7 + h, fins(2, h))
    sum_sent(2)
    sum_sent(3)
    for cp in copies:
        cp.wait()


def finish(q, f, own, shards, d_ref, u_ref, w_ref, v_ref, a_ref, b_ref, *outs):
    qkv_ref, out_ref, up_ref, down_ref, vec_ref, upb_ref, ao_ref, bo_ref, lines = outs
    ao_ref[...] = a_ref[...]
    bo_ref[...] = b_ref[...]
    width = 4 * q
    for i in range(4):
        down_ref[:, i * f : (i + 1) * f] = d_ref[i, :, 0:f].astype(F32)
        up_ref[:, i * f : (i + 1) * f] = u_ref[i, :, 0:f].astype(F32)
        out_ref[:, i * q : (i + 1) * q] = w_ref[i, :, 0:q].astype(F32)
        for k in range(3):
            start = k * width + i * q
            qkv_ref[:, start : start + q] = w_ref[i, :, (k + 1) * q : (k + 2) * q].astype(F32)

    @pl.when(pl.program_id(0) == 0)
    def _():
        lines[...] = v_ref[0] + v_ref[1] + v_ref[2] + v_ref[3]
        for i in range(4):
            upb_ref[:, i * f : (i + 1) * f] = v_ref[i, 3:4, 0:f]
        for i in range(4):
            lines[2:3, i * q : (i + 1) * q] = v_ref[i, 2:3, q : 2 * q]
            lines[3:4, i * q : (i + 1) * q] = v_ref[i, 2:3, 3 * q : 4 * q]
        shard = lax.axis_index("shard")
        for s in range(shards):

            @pl.when(shard == s)
            def _():
                vec_ref[...] = lines[:, s * own : (s + 1) * own]


def per_device(reps, shards, images, cotangent, w_qkv, w_out, w_up, w_down, vectors, up_bias):
    batch, seq, d = images.shape
    hidden = w_up.shape[1]
    q, f = d // reps, hidden // reps
    wide = -(-max(4 * q, f) // 128) * 128
    sub = shards // RING
    groups = [[i * sub + j for j in range(sub)] for i in range(RING)]
    own = d // shards
    weights = (w_qkv, w_out, w_up, w_down, vectors)
    if sub > 1:
        weights = tuple(
            lax.all_gather(w, "shard", axis=0, tiled=True, axis_index_groups=groups) for w in weights
        )
    c = Sizes(d, seq, wide, own * sub, sub, hidden)
    vmem = pl.BlockSpec(memory_space=pltpu.VMEM)
    hbm = pl.BlockSpec(memory_space=pl.ANY)
    grad = jax.ShapeDtypeStruct((4, c.b, wide), BF16)
    tok = jax.ShapeDtypeStruct((seq, d), BF16)
    outputs, input_grad, *terms, vf = pl.pallas_call(
        functools.partial(kernel, c),
        out_shape=(tok, tok, grad, grad, grad, jax.ShapeDtypeStruct((4, 8, d), F32)),
        in_specs=[hbm] * 4 + [vmem] * 4,
        out_specs=(hbm,) * 6,
        scratch_shapes=[make(c) for make in SCRATCH.values()],
        name="layer",
        compiler_params=pltpu.CompilerParams(
            collective_id=0, has_side_effects=True, vmem_limit_bytes=67043328
        ),
    )(*weights[:4], images.reshape(seq, d), cotangent.reshape(seq, d), weights[4].T, up_bias.reshape(1, hidden))
    if sub > 1:
        terms = [
            lax.psum_scatter(
                g.astype(F32), "shard", scatter_dimension=1, tiled=True, axis_index_groups=groups
            )
            for g in terms
        ]
        vf = lax.psum(vf, "shard", axis_index_groups=groups)
    steps = BANDS if own % (16 * BANDS) == 0 else 1
    rows = own // steps
    trow = -(-seq // (16 * steps)) * 16

    def lined(width):
        return pl.BlockSpec((rows, width), lambda j: (j, 0))

    part = pl.BlockSpec((4, rows, wide), lambda j: (0, j, 0))
    toks = pl.BlockSpec((trow, d), lambda j: (j, 0))

    def whole(*shape):
        return pl.BlockSpec(shape, lambda j: (0,) * len(shape))

    def f32(*shape):
        return jax.ShapeDtypeStruct(shape, F32)

    g_qkv, g_out, g_up, g_down, vec, upb, outputs, input_grad = pl.pallas_call(
        functools.partial(finish, q, f, own, shards),
        grid=(steps,),
        out_shape=(
            f32(own, 3 * d), f32(own, d), f32(own, hidden), f32(own, hidden), f32(8, own), f32(1, hidden), tok, tok
        ),
        in_specs=[part] * 3 + [whole(4, 8, d), toks, toks],
        out_specs=(
            lined(3 * d), lined(d), lined(hidden), lined(hidden), whole(8, own), whole(1, hidden), toks, toks
        ),
        scratch_shapes=[pltpu.VMEM((8, d), F32)],
        name="unpack",
    )(*terms, vf, outputs, input_grad)
    shape = (batch, seq, d)
    return (
        outputs.reshape(shape),
        input_grad.reshape(shape),
        g_qkv,
        g_out,
        g_up,
        g_down,
        vec.T,
        upb.reshape(hidden),
    )


def solution(mesh):
    reps, shards = mesh.shape["rep"], mesh.shape["shard"]
    token = P(("rep", "shard"), None, None)
    line = P("shard", None)

    def body(*args):
        return per_device(reps, shards, *args)

    return jax.shard_map(
        body,
        mesh=mesh,
        in_specs=(token, token, line, line, line, line, line, P()),
        out_specs=(token, token, line, line, line, line, line, P()),
        check_vma=False,
    )
```
